32 devices in a mesh: shard: 8 (over z, y), width: 4 (over x, core).
Axes of the slice: x: 2, y: 2, z: 4, core: 2. Of those that a mesh axis runs over, the one named last changes fastest.
Arguments:
- weight_gate: float32 [2048, 8192], P('shard', 'width'), may hold values from -0.1875 to 0.1875
- moment_gate: float32 [2048, 8192], P('shard', 'width'), may hold values from -6 to 6
- square_gate: float32 [2048, 8192], P('shard', 'width'), may hold values from 0.1 to 10
- weight_up: float32 [2048, 8192], P('shard', 'width'), may hold values from -0.1875 to 0.1875
- moment_up: float32 [2048, 8192], P('shard', 'width'), may hold values from -6 to 6
- square_up: float32 [2048, 8192], P('shard', 'width'), may hold values from 0.1 to 10
- norm_train: float32 [2048], P(('shard', 'width')), may hold values from 0.25 to 1.75
- norm_step: float32 [2048], P(('shard', 'width')), may hold values from -0.3 to 0.3
Outputs:
- serving_gate: bfloat16 [2048, 8192], P(None, 'width')
- serving_up: bfloat16 [2048, 8192], P(None, 'width')
- scale_gate: float32 [8192], P('width')
- scale_up: float32 [8192], P('width')
- serve_norm: bfloat16 [2048], replicated
- whole_gate: float32 [2048, 8192], P('shard', 'width')
- whole_up: float32 [2048, 8192], P('shard', 'width')
The draws below stay inside these ranges and needn't reach their ends.
All inputs are finite; a program needn't handle non-finite values. Where the reference program divides by a largest or mean magnitude, that divisor is 1e-20 or more.
Results may differ from the reference program's by a relative error of at most 0.001.
Values may be sent and summed in bfloat16 or wider, within the bound.
No kernel may reach another device: no remote copies, remote signals or barrier semaphores. Data moves between devices by JAX's collectives and lax.ppermute only.
A program may use at most 128 MiB of HBM per device.

```python
import math
import jax
import jax.numpy as jnp
from jax import lax

D_MODEL = 2048
D_INNER = 8192


def raised(entries, stream_key, source, target, blocks, factor):
    owner, partner = [(jnp.arange(entries.shape[dim]) // (entries.shape[dim] // blocks)).reshape([-1 if axis == dim else 1 for axis in range(entries.ndim)]) for dim in (source, target)]
    chosen = jax.random.permutation(stream_key, blocks)[partner]
    strong = (owner == chosen) | (owner == (partner + blocks // 2) % blocks)
    return jnp.where(strong, factor * entries, entries)


def shard_levels(stream_key, dims, cuts, low, high):
    level, own = 1.0, jax.random.fold_in(stream_key, 6)
    for axis_at, blocks in cuts:
        draws = jnp.exp(jax.random.uniform(jax.random.fold_in(own, axis_at), (blocks,), jnp.float32, low / len(cuts), high / len(cuts)))
        level = level * jnp.repeat(draws, dims[axis_at] // blocks).reshape([-1 if axis == axis_at else 1 for axis in range(len(dims))])
    return level


def scatter_about(stream_key, shape, scale, most, shards=(), held_as=jnp.bfloat16):
    values = scale * jax.random.normal(stream_key, shape, jnp.float32)
    if shards:
        values = values * shard_levels(stream_key, shape, shards, -0.22, 0.18)
    return jnp.clip(values, -most, most).astype(held_as)


def heavy_noise(key, extent, width, limit, pieces, heavy, kind=jnp.bfloat16):
    entries = width * jax.random.normal(key, extent, jnp.float32)
    if pieces:
        entries = entries * shard_levels(key, extent, pieces, -0.22, 0.18)
    return jnp.clip(raised(entries, jax.random.fold_in(key, 3), *heavy), -limit, limit).astype(kind)


def setup_inputs(seed: int = 0) -> dict:
    arg_keys = jax.random.split(jax.random.key(seed), 9)
    weight_gate = heavy_noise(arg_keys[0], (D_MODEL, D_INNER), D_MODEL ** -0.5, 0.1875, ((0, 8), (1, 4)), (0, 1, 8, 2.0), jnp.float32)
    moment_gate = scatter_about(arg_keys[1], (D_MODEL, D_INNER), 1.0, 6.0, ((0, 8), (1, 4)), jnp.float32)
    square_gate = jnp.clip(jnp.exp(math.log(10.0) - 4.6051702 * jax.random.uniform(arg_keys[2], (D_MODEL, D_INNER), jnp.float32) ** shard_levels(arg_keys[2], (D_MODEL, D_INNER), ((0, 8), (1, 4)), -0.2, 0.2)), 0.1, 10.0)
    weight_up = heavy_noise(arg_keys[3], (D_MODEL, D_INNER), D_MODEL ** -0.5, 0.1875, ((0, 8), (1, 4)), (0, 1, 8, 2.0), jnp.float32)
    moment_up = scatter_about(arg_keys[4], (D_MODEL, D_INNER), 1.0, 6.0, ((0, 8), (1, 4)), jnp.float32)
    square_up = jnp.clip(jnp.exp(math.log(10.0) - 4.6051702 * jax.random.uniform(arg_keys[5], (D_MODEL, D_INNER), jnp.float32) ** shard_levels(arg_keys[5], (D_MODEL, D_INNER), ((0, 8), (1, 4)), -0.2, 0.2)), 0.1, 10.0)
    norm_train = jnp.clip(1.0 + 0.15 * jax.random.normal(arg_keys[6], (D_MODEL,), jnp.float32), 0.25, 1.75)
    norm_step = jnp.clip(jax.random.uniform(arg_keys[7], (D_MODEL,), jnp.float32, -0.3, 0.3) * shard_levels(arg_keys[7], (D_MODEL,), ((0, 32),), -0.4, 0.0), -0.3, 0.3)
    return dict(weight_gate=weight_gate, moment_gate=moment_gate, square_gate=square_gate, weight_up=weight_up, moment_up=moment_up, square_up=square_up, norm_train=norm_train, norm_step=norm_step)


learn_rate = 0.02
decay_rate = 0.1
tiny_value = 1e-08

def reference(weight_gate, moment_gate, square_gate, weight_up, moment_up, square_up, norm_train, norm_step):
    whole_gate = weight_gate - learn_rate * (moment_gate / (jnp.sqrt(square_gate) + tiny_value) + decay_rate * weight_gate)
    whole_up = weight_up - learn_rate * (moment_up / (jnp.sqrt(square_up) + tiny_value) + decay_rate * weight_up)
    scale_gate = lax.optimization_barrier(jnp.max(jnp.abs(whole_gate), axis=0))
    serving_gate = (whole_gate / scale_gate).astype(jnp.bfloat16)
    scale_up = lax.optimization_barrier(jnp.max(jnp.abs(whole_up), axis=0))
    serving_up = (whole_up / scale_up).astype(jnp.bfloat16)
    serve_norm = (norm_train + norm_step).astype(jnp.bfloat16)
    return (serving_gate, serving_up, scale_gate, scale_up, serve_norm, whole_gate, whole_up)
```

```python
import jax
import jax.numpy as jnp
from jax import lax
from jax.sharding import PartitionSpec as P

learn_rate = 0.02
decay_rate = 0.1
tiny_value = 1e-08


def stepped(weight, moment, square):
    return weight - learn_rate * (moment / (jnp.sqrt(square) + tiny_value) + decay_rate * weight)


def largest_over(value, axis, size):
    if size & (size - 1):
        return lax.pmax(value, axis)
    bit = 1
    while bit < size:
        partner = [(i, i ^ bit) for i in range(size)]
        value = jnp.maximum(value, lax.ppermute(value, axis, partner))
        bit *= 2
    return value


def gather_rows(own, size):
    pair = 2 if size % 2 == 0 else 1
    line = size // pair
    index = lax.axis_index("shard")
    place, side = index // pair, index % pair
    across = [(i, i ^ 1) for i in range(size)]

    def down(hop):
        return [(i, i - pair) for i in range(pair, size) if i // pair + hop <= line]

    def up(hop):
        return [(i, i + pair) for i in range(size - pair) if i // pair - hop + 1 >= 0]

    count = len(own)
    below, above = [[block] for block in own], [[block] for block in own]
    mine = [[block] for block in own]
    other = [[lax.ppermute(block, "shard", across)] if pair == 2 else [] for block in own]
    for hop in range(1, line):
        for c in range(count):
            below[c].append(lax.ppermute(below[c][-1], "shard", down(hop)))
            above[c].append(lax.ppermute(above[c][-1], "shard", up(hop)))
        for c in range(count):
            turn = jnp.maximum(place - (line - 1 - hop), 0)
            block = below[c][hop]
            for back in range(1, hop + 1):
                block = jnp.where(turn == back, above[c][back], block)
            mine[c].append(block)
            if pair == 2:
                other[c].append(lax.ppermute(block, "shard", across))
    gathered = []
    for c in range(count):
        rows, columns = own[c].shape
        out = jnp.zeros((size * rows, columns), own[c].dtype)
        for hop in range(line):
            at = jnp.where(place <= line - 1 - hop, place + hop, line - 1 - hop) * pair
            out = lax.dynamic_update_slice(out, mine[c][hop], ((at + side) * rows, 0))
            if pair == 2:
                out = lax.dynamic_update_slice(out, other[c][hop], ((at + 1 - side) * rows, 0))
        gathered.append(out)
    return gathered


def make_body(shards, widths):
    def body(
        weight_gate, moment_gate, square_gate, weight_up, moment_up, square_up, norm_train, norm_step
    ):
        index = lax.axis_index("shard") * widths + lax.axis_index("width")
        part = norm_train.shape[0]
        norm = lax.dynamic_update_slice(
            jnp.full((part * shards * widths,), -jnp.inf, jnp.float32),
            norm_train + norm_step,
            (index * part,),
        )
        whole_gate = stepped(weight_gate, moment_gate, square_gate)
        columns = whole_gate.shape[1]
        sent = jnp.concatenate([jnp.max(jnp.abs(whole_gate), axis=0), norm])
        sent = largest_over(sent, "shard", shards)
        scale_gate, norm = sent[:columns], sent[columns:]
        narrow_gate = (whole_gate / scale_gate).astype(jnp.bfloat16)

        whole_up = stepped(weight_up, moment_up, square_up)
        scale_up = largest_over(jnp.max(jnp.abs(whole_up), axis=0), "shard", shards)
        narrow_up = (whole_up / scale_up).astype(jnp.bfloat16)

        serving_gate, serving_up = gather_rows([narrow_gate, narrow_up], shards)
        serve_norm = largest_over(norm, "width", widths).astype(jnp.bfloat16)
        return (serving_gate, serving_up, scale_gate, scale_up, serve_norm, whole_gate, whole_up)

    return body


def solution(mesh):
    cut = P("shard", "width")
    return jax.shard_map(
        make_body(mesh.shape["shard"], mesh.shape["width"]),
        mesh=mesh,
        in_specs=(cut, cut, cut, cut, cut, cut, P(("shard", "width")), P(("shard", "width"))),
        out_specs=(
            P(None, "width"),
            P(None, "width"),
            P("width"),
            P("width"),
            P(),
            cut,
            cut,
        ),
        check_vma=False,
    )
```
